256 devices in a mesh: dp: 8 (over x_hi, y), fsdp: 32 (over x_lo, z, core).
Axes of the slice: x: 4 (x_hi: 2, x_lo: 2; x = x_hi * 2 + x_lo), y: 4, z: 8, core: 2. Of those that a mesh axis runs over, the one named last changes fastest.
Arguments:
- inputs: bfloat16 [8, 64, 3584], P('dp', 'fsdp'), may hold values from -16 to 16
- baseline: bfloat16 [8, 64, 3584], P('dp', 'fsdp'), may hold values from -6 to 6
- cotangent: bfloat16 [8, 64, 3584], P('dp', 'fsdp'), may hold values from -6 to 6
- interval: int32 [8], P('dp'), may hold values from 0 to 7
- pre_gain: float32 [3584], replicated, may hold values from 0.1 to 1.9
- post_gain: float32 [3584], replicated, may hold values from 0.1 to 1.9
- gate_weight: bfloat16 [3584, 14336], P('dp', 'fsdp'), may hold values from -0.09375 to 0.09375
- up_weight: bfloat16 [3584, 14336], P('dp', 'fsdp'), may hold values from -0.09375 to 0.09375
- down_weight: bfloat16 [14336, 3584], P('fsdp', 'dp'), may hold values from -0.046875 to 0.046875
Outputs:
- attribution: float32 [8, 64, 3584], P('dp', 'fsdp')
The draws below stay inside these ranges and needn't reach their ends.
All inputs are finite; a program needn't handle non-finite values.
Results may differ from the reference program's by a relative error of at most 0.0027.
Values may be sent and summed in bfloat16 or wider, within the bound.
A program may use at most 64 MiB of HBM per device.

```python
import math
import jax
import jax.numpy as jnp
from jax import lax

D = 3584
FF = 14336
STEPS = 4
SPANS = 8
TOTAL = 32
PROMPTS = 8
SEQ = 64


def draw_inputs(key, part):
    key_rows, key_cols, key_vals = jax.random.split(key, 3)
    rows_scale = jnp.exp(jax.random.uniform(key_rows, (PROMPTS, SEQ, 1), jnp.float32, math.log(0.3), math.log(3.0)))
    cols_scale = jnp.exp(jax.random.uniform(key_cols, (1, 1, D), jnp.float32, math.log(0.4), math.log(2.5)))
    values = jax.random.normal(key_vals, (PROMPTS, SEQ, D), jnp.float32) * rows_scale * cols_scale
    return jnp.clip(values, -16.0, 16.0).astype(jnp.bfloat16)


def touch_ends(values, rng, smallest, top_value):
    index_at = [jax.random.randint(jax.random.fold_in(rng, axis), (), 0, length) for axis, length in enumerate(values.shape)]
    main_axis = values.shape.index(max(values.shape))
    neighbour = index_at[:main_axis] + [(index_at[main_axis] + 1) % values.shape[main_axis]] + index_at[main_axis + 1:]
    return values.at[tuple(index_at)].set(smallest).at[tuple(neighbour)].set(top_value)


def block_scale(own_key, extent, cuts, low, high):
    level, own = 1.0, jax.random.fold_in(own_key, 6)
    for position, shards_of in cuts:
        heights = jnp.exp(jax.random.uniform(jax.random.fold_in(own, position), (shards_of,), jnp.float32, low / len(cuts), high / len(cuts)))
        level = level * jnp.repeat(heights, extent[position] // shards_of).reshape([-1 if axis == position else 1 for axis in range(len(extent))])
    return level


def scatter_about(rng, extent, scale, most, cuts=(), dtype=jnp.bfloat16):
    result = jax.random.normal(rng, extent, jnp.float32) * scale
    if len(cuts) > 0:
        result = block_scale(rng, extent, cuts, -0.22, 0.18) * result
    return jnp.clip(result, min=-most, max=most).astype(dtype)


def setup_inputs(seed: int = 0) -> dict:
    arg_keys = jax.random.split(jax.random.key(seed), 10)
    inputs = draw_inputs(jax.random.fold_in(arg_keys[9], 71), 0)
    baseline = scatter_about(arg_keys[1], (PROMPTS, SEQ, D), 1.0, 6.0, ((0, 8), (1, 32)))
    cotangent = scatter_about(arg_keys[2], (PROMPTS, SEQ, D), 1.0, 6.0, ((0, 8), (1, 32)))
    interval = touch_ends(jax.random.randint(arg_keys[3], (PROMPTS,), 0, SPANS), jax.random.fold_in(arg_keys[3], 1), 0, SPANS - 1).astype(jnp.int32)
    pre_gain = jnp.clip(1.0 + 0.18 * jax.random.normal(arg_keys[4], (D,), jnp.float32), 0.1, 1.9)
    post_gain = jnp.clip(1.0 + 0.18 * jax.random.normal(arg_keys[5], (D,), jnp.float32), 0.1, 1.9)
    gate_weight = scatter_about(arg_keys[6], (D, FF), D ** -0.5, 0.09375, ((0, 8), (1, 32)))
    up_weight = scatter_about(arg_keys[7], (D, FF), D ** -0.5, 0.09375, ((0, 8), (1, 32)))
    down_weight = scatter_about(arg_keys[8], (FF, D), FF ** -0.5, 0.046875, ((0, 32), (1, 8)))
    return dict(inputs=inputs, baseline=baseline, cotangent=cotangent, interval=interval, pre_gain=pre_gain, post_gain=post_gain, gate_weight=gate_weight, up_weight=up_weight, down_weight=down_weight)


epsilon = 1e-06
root_coef = math.sqrt(2.0 / math.pi)

def gelu_parts(argument):
    tangent = jnp.tanh(root_coef * (argument + 0.044715 * argument * argument * argument))
    gelu_value = 0.5 * argument * (1.0 + tangent)
    gelu_slope = 0.5 * (1.0 + tangent) + 0.5 * argument * (1.0 - tangent * tangent) * root_coef * (1.0 + 3.0 * 0.044715 * argument * argument)
    return (gelu_value, gelu_slope)

def norm_back(grad_in, source, gain):
    scaled = grad_in * gain
    inverse = lax.rsqrt(lax.optimization_barrier(jnp.mean(source * source, axis=-1, keepdims=True)) + epsilon)
    inner_mean = lax.optimization_barrier(jnp.mean(scaled * source, axis=-1, keepdims=True))
    return inverse * (scaled - source * inverse * inverse * inner_mean)

def reference(inputs, baseline, cotangent, interval, pre_gain, post_gain, gate_weight, up_weight, down_weight):
    source = inputs.astype(jnp.float32)
    anchor = baseline.astype(jnp.float32)
    target = cotangent.astype(jnp.float32).reshape(-1, D)
    offset = source - anchor
    summed = jnp.zeros(source.shape, jnp.float32)
    starts = interval.astype(jnp.float32)[:, None, None]
    for step_index in range(STEPS):
        fraction = (starts * STEPS + (step_index + 0.5)) / TOTAL
        sample_point = anchor + fraction * offset
        inverse = lax.rsqrt(lax.optimization_barrier(jnp.mean(sample_point * sample_point, axis=-1, keepdims=True)) + epsilon)
        normed = (sample_point * inverse * pre_gain).astype(jnp.bfloat16).reshape(-1, D)
        gate_val = jnp.dot(normed, gate_weight, preferred_element_type=jnp.float32)
        up_val = jnp.dot(normed, up_weight, preferred_element_type=jnp.float32)
        gelu_value, gelu_slope = gelu_parts(gate_val)
        hidden = (gelu_value * up_val).astype(jnp.bfloat16)
        branch = jnp.dot(hidden, down_weight, preferred_element_type=jnp.float32)
        branch_grad = norm_back(target, branch, post_gain).astype(jnp.bfloat16)
        hidden_grad = jnp.dot(branch_grad, down_weight.T, preferred_element_type=jnp.float32)
        gate_grad = (hidden_grad * up_val * gelu_slope).astype(jnp.bfloat16)
        up_grad = (hidden_grad * gelu_value).astype(jnp.bfloat16)
        normed_grad = jnp.dot(gate_grad, gate_weight.T, preferred_element_type=jnp.float32) + jnp.dot(up_grad, up_weight.T, preferred_element_type=jnp.float32)
        summed = summed + norm_back(normed_grad.reshape(source.shape), sample_point, pre_gain)
    return offset * summed / STEPS
```

```python
import math

import jax
import jax.numpy as jnp
from jax import lax
from jax.experimental import pallas as pl
from jax.experimental.pallas import tpu as pltpu
from jax.sharding import PartitionSpec as P

STEPS = 4
TOTAL = 32
D = 3584
HID = 448
HALF = 224
CH = 896
KEEP = 384

epsilon = 1e-06
root_coef = math.sqrt(2.0 / math.pi)
bf16 = jnp.bfloat16
f32 = jnp.float32


def dot(a, b, dims):
    return lax.dot_general(a, b, (dims, ((), ())), preferred_element_type=f32)


NN = ((1,), (0,))
NT = ((1,), (1,))


def gelu_parts(argument):
    tangent = jnp.tanh(root_coef * (argument + 0.044715 * argument * argument * argument))
    gelu_value = 0.5 * argument * (1.0 + tangent)
    gelu_slope = 0.5 * (1.0 + tangent) + 0.5 * argument * (1.0 - tangent * tangent) * root_coef * (
        1.0 + 3.0 * 0.044715 * argument * argument
    )
    return (gelu_value, gelu_slope)


def kernel(
    gu_in, dt_in, nrm_in, r_in, u_in,
    t_out, m_out,
    gu, dt, nz, nx, rz, rx, part, xr, zs, zr, bsum, bg, agz, agx,
    pre, gval, gslp, ts, tx, tzs, tz, ms, mx, mzs, mz,
    w_send, g_hop, g_y, g_dd, d_hop, d_y, d_dd,
    nz_s, nz_r, nx_s, nx_r, rz_s, rz_r, rx_s, rx_r,
    xs_s, xs_r, zs_s, zs_r, az_s, az_r, ax_s, ax_r,
    tx_s, tx_r, tz_s, tz_r, mx_s, mx_r, mz_s, mz_r,
):
    dp = lax.axis_index("dp")
    fs = lax.axis_index("fsdp")
    xh, y = dp // 4, dp % 4
    xl, z, co = fs // 16, (fs // 2) % 8, fs % 2
    x = xh * 2 + xl

    def dev(x_, y_, z_, c_):
        return ((x_ // 2) * 4 + y_, ((x_ % 2) * 8 + z_) * 2 + c_)

    barrier = pltpu.get_barrier_semaphore()
    peers = [dev((x + i) % 4, y, z, (co + j) % 2) for i in range(4) for j in range(2) if i or j]
    peers += [dev(x, y, (z + i) % 8, co) for i in range(1, 8)]
    peers += [dev(x, (y + i) % 4, z, co) for i in (1, 3)]
    for peer in peers:
        pl.semaphore_signal(barrier, inc=1, device_id=peer, device_id_type=pl.DeviceIdType.MESH)
    pl.semaphore_wait(barrier, len(peers))

    pending = []

    def send(src, dst, s_sem, r_sem, to):
        c = pltpu.make_async_remote_copy(
            src_ref=src, dst_ref=dst, send_sem=s_sem, recv_sem=r_sem,
            device_id=to, device_id_type=pl.DeviceIdType.MESH,
        )
        c.start()
        return c

    def arrived(ref, sem):
        pltpu.make_async_copy(ref, ref, sem).wait()

    def to_z(src_of, dst, s_sem, r_sem):
        for i in range(1, 8):
            to = (z + i) % 8
            send(src_of(to), dst.at[i - 1], s_sem, r_sem, dev(x, y, to, co))
        pending.append((dst.at[pl.ds(0, 7)], s_sem))

    up_y = dev(x, (y + 1) % 4, z, co)
    down_y = dev(x, (y + 3) % 4, z, co)
    mate = dev(x, y, z, 1 - co)
    owner = dev(2 * co + 1 - xl, y, z, xh)

    class Weights:
        def __init__(self, src, buf, hop, ring, dd, base):
            self.src, self.buf, self.hop, self.ring, self.dd, self.base = src, buf, hop, ring, dd, base
            self.sent = 0

        def put(self, src, s, h, p, sem, to):
            c = send(src, self.buf.at[s, h, p], w_send.at[self.base + self.sent], sem, to)
            self.sent += 1
            pending.append((src, w_send.at[self.base + self.sent - 1]))

        def start(self):
            for p in range(2):
                self.put(self.src.at[p], 0, xh, p, self.hop.at[p], owner)

        def wait_hop(self, p):
            arrived(self.buf.at[0, co, p], self.hop.at[p])

        def wait_ring(self, s, p):
            arrived(self.buf.at[s, co, p], self.ring.at[s - 1, p])

        def up(self, p):
            self.put(self.buf.at[0, co, p], 2, co, p, self.ring.at[1, p], up_y)

        def down(self, p):
            self.put(self.buf.at[0, co, p], 1, co, p, self.ring.at[0, p], down_y)

        def relay_up(self):
            self.put(self.buf.at[2, co, 0], 3, co, 0, self.ring.at[2, 0], up_y)

        def relay_down(self):
            self.put(self.buf.at[1, co, 1], 3, co, 1, self.ring.at[2, 1], down_y)

        def share(self, s, p):
            self.put(self.buf.at[s, co, p], s, co, p, self.dd.at[s, p], mate)

        def wait_share(self, s):
            for p in range(2):
                arrived(self.buf.at[s, 1 - co, p], self.dd.at[s, p])

    g = Weights(gu_in, gu, g_hop, g_y, g_dd, 0)
    d = Weights(dt_in, dt, d_hop, d_y, d_dd, 16)

    g.start()
    to_z(lambda to: nrm_in, nz, nz_s, nz_r)
    to_z(lambda to: r_in, rz, rz_s, rz_r)

    home_slot = xl * 2 + co

    def to_workers(src, copies, slot_of, s_sem, r_sem):
        own = co == xh
        slot = slot_of(home_slot)
        for i in range(4):
            to = dev((x + i) % 4, y, z, xh)
            if i == 0:
                @pl.when(jnp.logical_not(own))
                def _():
                    send(src, slot, s_sem.at[0], r_sem.at[home_slot], to)

                @pl.when(own)
                def _():
                    copies()
            else:
                send(src, slot, s_sem.at[i], r_sem.at[home_slot], to)
                pending.append((src, s_sem.at[i]))
        late.append((jnp.logical_not(own), src, s_sem.at[0]))

    late = []

    def from_homes(slot_of, r_sem):
        for i in range(4):
            mine = jnp.logical_and(xh == co, home_slot == i)

            @pl.when(jnp.logical_not(mine))
            def _():
                arrived(slot_of(i), r_sem.at[i])

    def to_homes(src_of, copies, slot_of, s_sem, r_sem):
        for i in range(4):
            l, a = i // 2, i % 2
            hx = 2 * co + l
            gap = (hx - x + 4) % 4
            own = jnp.logical_and(gap == 0, co == a)
            to = dev(hx, y, z, a)

            @pl.when(jnp.logical_not(own))
            def _():
                send(src_of(i), slot_of(gap), s_sem.at[i], r_sem.at[gap], to)

            @pl.when(own)
            def _():
                copies(i)
            late.append((jnp.logical_not(own), src_of(i), s_sem.at[i]))

    def from_workers(slot_of, r_sem):
        own = co == xh
        for i in range(4):
            if i == 0:
                @pl.when(jnp.logical_not(own))
                def _():
                    arrived(slot_of(0), r_sem.at[0])
            else:
                arrived(slot_of(i), r_sem.at[i])

    g.wait_hop(0)
    g.up(0)
    g.share(0, 0)
    g.wait_hop(1)
    g.down(1)
    g.up(1)
    g.down(0)
    g.share(0, 1)

    arrived(nz.at[pl.ds(0, 7)], nz_r)
    arrived(rz.at[pl.ds(0, 7)], rz_r)
    nz[7] = nrm_in[...]
    rz[7] = r_in[...]

    def copy_n():
        nx[home_slot] = nz[...]

    def copy_r():
        rx[home_slot] = rz[...]

    to_workers(nz, copy_n, lambda i: nx.at[i], nx_s, nx_r)
    to_workers(rz, copy_r, lambda i: rx.at[i], rx_s, rx_r)
    d.start()

    g.wait_ring(2, 0)
    g.relay_up()
    g.share(2, 0)
    g.wait_ring(1, 1)
    g.relay_down()
    g.share(1, 1)
    d.wait_hop(0)
    d.up(0)
    d.share(0, 0)
    d.wait_hop(1)
    d.down(1)
    d.up(1)
    d.down(0)
    d.share(0, 1)
    g.wait_ring(2, 1)
    g.share(2, 1)
    g.wait_ring(1, 0)
    g.share(1, 0)

    from_homes(lambda i: nx.at[i], nx_r)
    from_homes(lambda i: rx.at[i], rx_r)

    chunk = [y, (y + 1) % 4, (y + 3) % 4, (y + 2) % 4]

    def rows_of(value):
        return value.astype(f32).reshape(256, CH).astype(bf16)

    for s in range(4):
        if s == 3:
            for p in range(2):
                g.wait_ring(3, p)
                g.share(3, p)
        g.wait_share(s)
        lhs = rows_of(nx[:, :, chunk[s]])
        add = dot(lhs, gu[s].reshape(CH, CH), NN)
        if s == 0:
            pre[...] = add
        else:
            pre[...] += add

    lane = lax.broadcasted_iota(jnp.int32, (256, 128), 1)

    def gate_of(v):
        return jnp.concatenate([v[:, :KEEP], v[:, 2 * KEEP :]], axis=1)

    def up_of(v):
        return jnp.concatenate([v[:, KEEP : 2 * KEEP], pltpu.roll(v[:, 2 * KEEP :], 64, 1)], axis=1)

    value, slope = gelu_parts(gate_of(pre[...]))
    gval[...] = value
    gslp[...] = slope
    hidden = (value * up_of(pre[...])).astype(bf16)[:, :HID]

    d.wait_ring(2, 0)
    d.relay_up()
    d.share(2, 0)
    d.wait_ring(1, 1)
    d.relay_down()
    d.share(1, 1)

    def branch(s):
        d.wait_share(s)
        part[s] = dot(hidden, dt[s].reshape(CH, HID), NT).astype(bf16).reshape(4, 64, CH)

        def copies(i):
            xr[s, 0] = part[s, i]

        to_homes(lambda i: part.at[s, i], copies, lambda i: xr.at[s, i], xs_s.at[s], xs_r.at[s])

    def middle(s):
        from_workers(lambda i: xr.at[s, i], xs_r.at[s])
        total = xr[s, 0].astype(f32) + xr[s, 1].astype(f32) + xr[s, 2].astype(f32) + xr[s, 3].astype(f32)
        for i in range(8):
            zs[s, i] = total[8 * i : 8 * i + 8].astype(bf16)
        for i in range(1, 8):
            send(zs.at[s, 7 - i], zr.at[s, 7 - i], zs_s.at[s], zs_r.at[s], dev(x, y, (z + i) % 8, co))
        pending.append((zs.at[s, pl.ds(0, 7)], zs_s.at[s]))

    branch(0)
    d.wait_ring(2, 1)
    d.share(2, 1)
    d.wait_ring(1, 0)
    d.share(1, 0)
    branch(1)
    branch(2)
    middle(0)
    middle(1)
    for p in range(2):
        d.wait_ring(3, p)
        d.share(3, p)
    branch(3)
    middle(2)
    middle(3)
    squares = jnp.zeros((8, 1), f32)
    inner = jnp.zeros((8, 1), f32)
    for s in range(4):
        arrived(zr.at[s, pl.ds(0, 7)], zs_r.at[s])
        total = zs[s, 7].astype(f32)
        for i in range(7):
            total = total + zr[s, i].astype(f32)
        bsum[s] = total
        squares = squares + jnp.sum(total * total, axis=-1, keepdims=True)
        inner = inner + jnp.sum(total * u_in[chunk[s]], axis=-1, keepdims=True)
    inverse = lax.rsqrt(squares * (1.0 / D) + epsilon)
    inner = inner * (1.0 / D)
    for s in range(4):
        bg[s] = (inverse * (u_in[chunk[s]] - bsum[s] * inverse * inverse * inner)).astype(bf16)
        to_z(lambda to: bg.at[s], agz.at[s], az_s.at[s], az_r.at[s])
    for s in range(4):
        arrived(agz.at[s, pl.ds(0, 7)], az_r.at[s])
        agz[s, 7] = bg[s]

        def copies():
            agx[s, home_slot] = agz[s]

        to_workers(agz.at[s], copies, lambda i: agx.at[s, i], ax_s.at[s], ax_r.at[s])

    for s in range(4):
        from_homes(lambda i: agx.at[s, i], ax_r.at[s])
        add = dot(rows_of(agx[s]), dt[s].reshape(CH, HID), NN)
        hg = add if s == 0 else hg + add
    hg = jnp.concatenate([hg, jnp.zeros((256, 64), f32)], axis=1)
    gate_grad = (hg * up_of(pre[...]) * gslp[...]).astype(bf16).astype(f32)
    up_grad = (hg * gval[...]).astype(bf16).astype(f32)
    last = jnp.where(lane < 64, gate_grad[:, KEEP:], pltpu.roll(up_grad[:, KEEP:], 64, 1))
    grads = jnp.concatenate([gate_grad[:, :KEEP], up_grad[:, :KEEP], last], axis=1)
    inner = jnp.sum(grads * pre[...], axis=-1, keepdims=True)
    weighted = grads * rx[...].reshape(256, 128)[:, :1]
    token = lax.broadcasted_iota(jnp.int32, (64, 256), 0)
    row = lax.broadcasted_iota(jnp.int32, (64, 256), 1)
    same = jnp.logical_and(row // 8 == token // 2, row % 2 == token % 2)
    pick = jnp.where(same, 1.0, 0.0).astype(bf16)
    high = weighted.astype(bf16)
    low = (weighted - high.astype(f32)).astype(bf16)
    summed = dot(pick, high, NN) + dot(pick, low, NN)
    high = summed.astype(bf16)
    low = (summed - high.astype(f32)).astype(bf16)
    both = jnp.concatenate([high, low], axis=0)

    lane8 = lax.broadcasted_iota(jnp.int32, (8, 128), 1)
    for i in range(4):
        tile = jnp.zeros((8, 128), f32)
        for j in range(8):
            at = i * 64 + j * 8
            tile = jnp.where(lane8 == j, inner[at : at + 8], tile)
        ms[i] = tile

    def copy_m(i):
        mx[0] = ms[i]

    to_homes(lambda i: ms.at[i], copy_m, lambda i: mx.at[i], mx_s, mx_r)

    for s in range(4):
        out = dot(both, gu[s].reshape(CH, CH), NT)
        ts[s] = (out[:64] + out[64:]).reshape(4, 16, CH)

        def copies(i):
            tx[s, 0] = ts[s, i]

        to_homes(lambda i: ts.at[s, i], copies, lambda i: tx.at[s, i], tx_s.at[s], tx_r.at[s])

    from_workers(lambda i: mx.at[i], mx_r)
    mzs[...] = mx[0] + mx[1] + mx[2] + mx[3]
    to_z(lambda to: mzs, mz, mz_s, mz_r)
    for s in range(4):
        from_workers(lambda i: tx.at[s, i], tx_r.at[s])
        total = tx[s, 0] + tx[s, 1] + tx[s, 2] + tx[s, 3]
        for i in range(8):
            tzs[s, i] = total[2 * i : 2 * i + 2]
        for i in range(1, 8):
            send(tzs.at[s, 7 - i], tz.at[s, 7 - i], tz_s.at[s], tz_r.at[s], dev(x, y, (z + i) % 8, co))
        pending.append((tzs.at[s, pl.ds(0, 7)], tz_s.at[s]))

    arrived(mz.at[pl.ds(0, 7)], mz_r)
    total = jnp.where(lane8 == 7, mzs[...], 0.0)
    for i in range(7):
        total = total + jnp.where(lane8 == 6 - i, mz[i], 0.0)
    m_out[...] = jnp.broadcast_to(jnp.sum(total, axis=-1, keepdims=True), (8, 128))
    for s in range(4):
        arrived(tz.at[s, pl.ds(0, 7)], tz_r.at[s])
        total = tzs[s, 7]
        for i in range(7):
            total = total + tz[s, i]
        t_out[chunk[s]] = total

    for ref, sem in pending:
        arrived(ref, sem)
    for cond, ref, sem in late:
        @pl.when(cond)
        def _():
            arrived(ref, sem)


def fold(rows):
    n = rows.shape[0]
    return rows.reshape(n, 2, 4, HID).transpose(2, 0, 1, 3).reshape(4, n, CH)


def per_device(
    inputs, baseline, cotangent, interval, pre_gain, post_gain, gate_weight, up_weight, down_weight
):
    anchor = baseline[0].astype(f32)
    offset = inputs[0].astype(f32) - anchor
    steps = jnp.arange(STEPS, dtype=f32) + 0.5
    fraction = (interval[0].astype(f32) * STEPS + steps) / TOTAL
    point = (anchor[None] + fraction[:, None, None] * offset[None]).reshape(8, D)
    inverse = lax.rsqrt(jnp.mean(point * point, axis=-1, keepdims=True) + epsilon)
    normed = fold((point * inverse * pre_gain).astype(bf16))
    scaled = fold(jnp.tile(cotangent[0].astype(f32) * post_gain, (4, 1)))
    gu = jnp.concatenate(
        [gate_weight[:, :KEEP], up_weight[:, :KEEP], gate_weight[:, KEEP:], up_weight[:, KEEP:]], axis=1
    ).reshape(2, HALF, CH)
    dt = down_weight.T.reshape(2, HALF, HID)
    vmem = pl.BlockSpec(memory_space=pltpu.VMEM)
    V = pltpu.VMEM
    dma = pltpu.SemaphoreType.DMA
    t, m = pl.pallas_call(
        kernel,
        out_shape=(jax.ShapeDtypeStruct((4, 2, CH), f32), jax.ShapeDtypeStruct((8, 128), f32)),
        in_specs=[vmem] * 5,
        out_specs=(vmem, vmem),
        scratch_shapes=[
            V((4, 2, 2, HALF, CH), bf16), V((4, 2, 2, HALF, HID), bf16),
            V((8, 4, 8, CH), bf16), V((4, 8, 4, 8, CH), bf16), V((8, 8, 128), f32), V((4, 8, 8, 128), f32),
            V((4, 4, 64, CH), bf16), V((4, 4, 64, CH), bf16), V((4, 8, 8, CH), bf16), V((4, 7, 8, CH), bf16),
            V((4, 8, CH), f32), V((4, 8, CH), bf16), V((4, 8, 8, CH), bf16), V((4, 4, 8, 8, CH), bf16),
            V((256, CH), f32), V((256, 512), f32), V((256, 512), f32),
            V((4, 4, 16, CH), f32), V((4, 4, 16, CH), f32), V((4, 8, 2, CH), f32), V((4, 7, 2, CH), f32),
            V((4, 8, 128), f32), V((4, 8, 128), f32), V((8, 128), f32), V((8, 8, 128), f32),
            dma((32,)), dma((2,)), dma((3, 2)), dma((4, 2)), dma((2,)), dma((3, 2)), dma((4, 2)),
            dma, dma, dma((4,)), dma((4,)), dma, dma, dma((4,)), dma((4,)),
            dma((4, 4)), dma((4, 4)), dma((4,)), dma((4,)), dma((4,)), dma((4,)), dma((4, 4)), dma((4, 4)),
            dma((4, 4)), dma((4, 4)), dma((4,)), dma((4,)), dma((4,)), dma((4,)), dma, dma,
        ],
        compiler_params=pltpu.CompilerParams(
            collective_id=0, has_side_effects=True, vmem_limit_bytes=60 * 1024 * 1024
        ),
    )(gu, dt, normed, jnp.broadcast_to(inverse, (8, 128)), scaled)
    along = t.reshape(4, 2, 2, HID).transpose(1, 2, 0, 3).reshape(2, D)
    weight = inverse * inverse * m[:, :1] * (1.0 / D)
    across = jnp.sum((point * weight).reshape(4, 2, D), axis=0)
    return (offset * (along * pre_gain - across) / STEPS)[None]


def solution(mesh):
    return jax.shard_map(
        per_device,
        mesh=mesh,
        in_specs=(
            P("dp", "fsdp", None),
            P("dp", "fsdp", None),
            P("dp", "fsdp", None),
            P("dp"),
            P(),
            P(),
            P("dp", "fsdp"),
            P("dp", "fsdp"),
            P("fsdp", "dp"),
        ),
        out_specs=P("dp", "fsdp", None),
        check_vma=False,
    )
```
